64 devices in a mesh: dp: 8 (over x, y, core), sp: 8 (over z).
Axes of the slice: x: 2, y: 2, z: 8, core: 2. Of those that a mesh axis runs over, the one named last changes fastest.
The devices are a block of a 4x4x8 slice.
Arguments:
- x: bfloat16 [16384, 4096], P(('dp', 'sp')), parts along dimension 0
- gain: bfloat16 [4096], replicated
- wq: bfloat16 [4096, 6144], replicated
- wk: bfloat16 [4096, 1024], replicated
- wv: bfloat16 [4096, 1024], replicated
- wo: bfloat16 [6144, 4096], replicated
Outputs:
- output: bfloat16 [16384, 4096], P(('dp', 'sp')), parts along dimension 0
There are 8 independent parts. The reference program is written for one: setup_inputs(seed, part) draws one part's arguments, and reference() takes and returns one part's arrays. A program takes and returns all parts, laid end to end along the dimension named above; an argument that names none is the same for every part.
All inputs are finite; a program needn't handle non-finite values.
Results may differ from the reference program's by a relative error of at most 0.012.
Values are sent between devices in bfloat16 or wider.
A program may use at most 768 MiB of HBM per device.

```python
import jax
import jax.numpy as jnp
from jax import lax

ROWS = 2048
D = 4096
HEADS = 48
KV_HEADS = 8
HEAD = 128
THETA = 10000


def setup_inputs(seed: int = 0, part: int = 0) -> dict:
    kx, kn, kq, kk, kv, ko = jax.random.split(jax.random.key(seed), 6)

    def weights(key, rows, columns):
        return jax.random.normal(key, (rows, columns), jnp.float32) * rows**-0.5

    drawn = {
        "x": jax.random.normal(jax.random.fold_in(kx, part), (ROWS, D), jnp.float32),
        "gain": 1 + 0.1 * jax.random.normal(kn, (D,), jnp.float32),
        "wq": 2 * weights(kq, D, HEADS * HEAD),
        "wk": 2 * weights(kk, D, KV_HEADS * HEAD),
        "wv": 4 * weights(kv, D, KV_HEADS * HEAD),
        "wo": weights(ko, HEADS * HEAD, D),
    }
    return {k: v.astype(jnp.bfloat16) for k, v in drawn.items()}


def normed(x, gain):
    wide = x.astype(jnp.float32)
    scale = lax.rsqrt(jnp.mean(wide * wide, -1, keepdims=True) + 1e-6)
    return (wide * scale * gain.astype(jnp.float32)).astype(jnp.bfloat16)


def turned(t, place, theta):
    half = t.shape[-1] // 2
    angle = place.astype(jnp.float32)[:, None] * theta ** (-jnp.arange(half, dtype=jnp.float32) / half)
    cos, sin = jnp.cos(angle)[:, None], jnp.sin(angle)[:, None]
    a, b = t[..., :half].astype(jnp.float32), t[..., half:].astype(jnp.float32)
    return jnp.concatenate([a * cos - b * sin, b * cos + a * sin], -1).astype(jnp.bfloat16)


def matmul(a, w):
    return jnp.dot(a, w, preferred_element_type=jnp.float32).astype(jnp.bfloat16)


def einsum(form, a, b):
    return jnp.einsum(form, a.astype(jnp.float32), b.astype(jnp.float32))


def attention(q, k, v):
    scores = einsum("tgsd,ugd->gstu", q, k) * q.shape[-1] ** -0.5
    token = jnp.arange(q.shape[0])
    scores = jnp.where(token[:, None] >= token, scores, -jnp.inf)
    weights = jax.nn.softmax(scores, -1).astype(jnp.bfloat16)
    return einsum("gstu,ugd->tgsd", weights, v).astype(jnp.bfloat16)


def reference(x, gain, wq, wk, wv, wo):
    a, place = normed(x, gain), jnp.arange(ROWS)
    q = turned(matmul(a, wq).reshape(ROWS, HEADS, HEAD), place, THETA).reshape(ROWS, KV_HEADS, -1, HEAD)
    k = turned(matmul(a, wk).reshape(ROWS, KV_HEADS, HEAD), place, THETA)
    v = matmul(a, wv).reshape(ROWS, KV_HEADS, HEAD)
    seen = attention(q, k, v).reshape(ROWS, HEADS * HEAD)
    return (x.astype(jnp.float32) + jnp.dot(seen, wo, preferred_element_type=jnp.float32)).astype(jnp.bfloat16)
```

```python
import functools

import jax
import jax.numpy as jnp
from jax import lax
from jax.experimental import pallas as pl
from jax.experimental.pallas import tpu as pltpu
from jax.sharding import PartitionSpec as P

HEAD = 128
THETA = 10000
LOG2E = 1.4426950408889634
HIDDEN = -2e30
WIDE = 256
STRIP = 512
SLOTS = 5


def _dot(a, b):
    return lax.dot_general(a, b, (((1,), (0,)), ((), ())), preferred_element_type=jnp.float32)


def _kernel(n, heads, group, cos_ref, sin_ref, gain_ref, x_hbm, wq, wk, wv, wo, out_ref,
            x_v, a_v, q_v, kv, y_v, top_s, mix_s, o_v, part_s, wbuf, wsem, xsem, ssem, rsem):
    me = lax.axis_index("sp")
    right, left = lax.rem(me + 1, n), lax.rem(me + n - 1, n)
    own, d = x_v.shape
    half = n // 2
    pairs = heads // 2
    gw = group * HEAD
    cols = group * own
    bf = jnp.bfloat16

    def pieces(kind, i, slot):
        if kind == "kv":
            at = pl.ds(i * WIDE, WIDE)
            return [pltpu.make_async_copy(w.at[:, at], wbuf.at[slot, pl.ds(j * d, d), :], wsem.at[slot, j]) for j, w in enumerate((wk, wv))]
        if kind == "q":
            return [pltpu.make_async_copy(wq.at[:, pl.ds(pl.multiple_of(i * gw + j * WIDE, WIDE), WIDE)], wbuf.at[slot, pl.ds(j * d, d), :],
                                          wsem.at[slot, j]) for j in range(gw // WIDE)]
        return [pltpu.make_async_copy(wo.at[pl.ds(pl.multiple_of(i * gw, gw), gw), pl.ds(j * WIDE, WIDE)],
                                      wbuf.at[slot, pl.ds(j * gw, gw), :], wsem.at[slot, j]) for j in range(d // WIDE)]

    def start(kind, i, slot):
        for c in pieces(kind, i, slot):
            c.start()

    def wait(kind, i, slot):
        for c in pieces(kind, i, slot):
            c.wait()

    xin = pltpu.make_async_copy(x_hbm, x_v, xsem.at[0])
    xin.start()
    start("kv", 0, 0)
    start("kv", 1, 1)

    barrier = pltpu.get_barrier_semaphore()
    for who in (left, right):
        pl.semaphore_signal(barrier, inc=1, device_id={"sp": who}, device_id_type=pl.DeviceIdType.MESH)
    pl.semaphore_wait(barrier, 2)

    xin.wait()

    def squares(i, _):
        rows = pl.ds(pl.multiple_of(i * 16, 16), 16)
        total = jnp.zeros((16, 128), jnp.float32)
        for c in range(0, d, 128):
            w = x_v[rows, c : c + 128].astype(jnp.float32)
            total += w * w
        part_s[rows, :] = total

    lax.fori_loop(0, own // 16, squares, None)
    part_s[...] = jnp.broadcast_to(lax.rsqrt(jnp.sum(part_s[...], -1, keepdims=True) * (1 / d) + 1e-6), part_s.shape)

    def scaled(i, _):
        rows = pl.ds(pl.multiple_of(i * 16, 16), 16)
        s = part_s[rows, :]
        for c in range(0, d, 128):
            a_v[rows, c : c + 128] = (x_v[rows, c : c + 128].astype(jnp.float32) * s * gain_ref[:, c : c + 128].astype(jnp.float32)).astype(bf)

    lax.fori_loop(0, own // 16, scaled, None)
    for p in range(2, pairs):
        start("kv", p, p)
    for g in range(SLOTS - pairs):
        start("q", g, pairs + g)

    def turned(t):
        t = t.astype(bf).astype(jnp.float32)
        return (t * cos_ref[...] + pltpu.roll(t, HEAD // 2, 1) * sin_ref[...]).astype(bf)

    def project(p):
        wait("kv", p, p)
        k = _dot(a_v[...], wbuf[p, :d, :])
        v = _dot(a_v[...], wbuf[p, d : 2 * d, :])
        for j in range(2):
            at = slice(j * HEAD, (j + 1) * HEAD)
            kv[2 * p + j, me, 0] = turned(k[:, at])
            low = v[:, at].astype(bf)
            for r in range(0, own, HEAD):
                kv[2 * p + j, me, 1, r : r + HEAD, :] = low[r : r + HEAD].T
        g = SLOTS - pairs + p
        start("q", g, p)

    def send(h, s, up):
        block = lax.rem(me - s + n, n) if up else lax.rem(me + s, n)
        ref = kv.at[h, block]
        if s == half - 1:
            ref = ref.at[0 if up else 1]
        return pltpu.make_async_remote_copy(src_ref=ref, dst_ref=ref, send_sem=ssem.at[int(up), h, s], recv_sem=rsem.at[int(up), h, s],
                                            device_id={"sp": right if up else left}, device_id_type=pl.DeviceIdType.MESH)

    def arrival(h, s, up):
        block = lax.rem(me - 1 - s + n, n) if up else lax.rem(me + 1 + s, n)
        ref = kv.at[h, block]
        if s == half - 1:
            ref = ref.at[0 if up else 1]
        return pltpu.make_async_remote_copy(src_ref=ref, dst_ref=ref, send_sem=ssem.at[int(up), h, s], recv_sem=rsem.at[int(up), h, s],
                                            device_id={"sp": left if up else right}, device_id_type=pl.DeviceIdType.MESH)

    def sends(s, up):
        return (me >= s) & (me < n - 1) if up else lax.rem(me + s, n) < half

    def receives(s, up):
        return me >= s + 1 if up else lax.rem(me + 1 + s, n) < half

    def hop(h, s):
        for up in (True, False):
            if s:
                @pl.when(receives(s - 1, up))
                def _():
                    arrival(h, s - 1, up).wait_recv()
            if s < half:
                @pl.when(sends(s, up))
                def _():
                    send(h, s, up).start()

    project(0)
    project(1)
    hop(0, 0)
    for p in range(2, pairs):
        project(p)

    def residual(i, _):
        rows = pl.ds(pl.multiple_of(i * 16, 16), 16)
        y_v[rows, :] = x_v[rows, :].astype(jnp.float32)

    lax.fori_loop(0, own // 16, residual, None)

    def queries(g):
        slot = lax.rem(pairs + g, SLOTS)
        wait("q", g, slot)
        for c in range(gw // WIDE):
            q = _dot(a_v[...], wbuf[slot, c * d : (c + 1) * d, :])
            for j in range(WIDE // HEAD):
                at = c * (WIDE // HEAD) + j
                q_v[g, :, at * own : (at + 1) * own] = turned(q[:, j * HEAD : (j + 1) * HEAD]).T
        nxt = g + SLOTS

        @pl.when(nxt < heads)
        def _():
            start("q", nxt, slot)

        @pl.when(nxt >= heads)
        def _():
            start("o", nxt - heads, slot)

    e = HEAD**-0.5 * LOG2E
    ones = jnp.ones((8, own), bf)

    def attend(h, block, first):
        k = kv[h, block, 0]
        values = jnp.concatenate([kv[h, block, 1, r : r + HEAD, :] for r in range(0, own, HEAD)], axis=1)
        values = jnp.concatenate([values, ones], axis=0)
        strips = range(0, cols, STRIP)
        scores = [_dot(k, q_v[h, :, at : at + STRIP]) for at in strips]
        weights, keeps = [], []
        for at, s in zip(strips, scores):
            if first:
                query = lax.rem(lax.broadcasted_iota(jnp.int32, s.shape, 1), own)
                s = jnp.where(query >= lax.broadcasted_iota(jnp.int32, s.shape, 0), s, HIDDEN)
                top = s.max(axis=0, keepdims=True)
            else:
                old = top_s[:, at : at + STRIP]
                top = jnp.maximum(old, s.max(axis=0, keepdims=True))
                keeps.append(jnp.exp2((old - top) * e))
            top_s[:, at : at + STRIP] = top
            weights.append(jnp.exp2((s - top) * e).astype(bf))
        for i, at in enumerate(strips):
            new = _dot(values, weights[i])
            mix_s[:, at : at + STRIP] = new if first else mix_s[:, at : at + STRIP] * keeps[i] + new

    def attend_most(h):
        attend(h, me, True)

        def one(i, _):
            far = i + 1 + (i >= half - 1).astype(jnp.int32)
            attend(h, me - far, False)

        lax.fori_loop(0, me - (me >= half).astype(jnp.int32), one, None)

    def finish(h):
        @pl.when(me >= half)
        def _():
            attend(h, me - half, False)

        for j in range(group):
            at = slice(j * own, (j + 1) * own)
            o = mix_s[:HEAD, at] * (1 / mix_s[HEAD : HEAD + 1, at])
            o_v[:, j * HEAD : (j + 1) * HEAD] = o.astype(bf).T
        slot = lax.rem(pairs + heads + h, SLOTS)
        wait("o", h, slot)

        def out(i, _):
            for j in range(4):
                piece = wbuf[slot, pl.ds(pl.multiple_of((i * 4 + j) * gw, gw), gw), :]
                at = pl.ds(pl.multiple_of((i * 4 + j) * WIDE, WIDE), WIDE)
                y_v[:, at] += _dot(o_v[...], piece)

        lax.fori_loop(0, d // WIDE // 4, out, None)

        @pl.when(h + SLOTS < heads)
        def _():
            start("o", h + SLOTS, slot)

    def when_head(h, do):
        @pl.when((h >= 0) & (h < heads))
        def _():
            do(h)

    per = 2

    def round_(t, _):
        when_head(jnp.where(t > 0, t, -1), lambda h: hop(h, 0))
        for i in range(per):
            if i == 1:
                when_head(t - 1, lambda h: hop(h, 1))
            when_head(t * per + i, queries)
        for s in range(2, half):
            when_head(t - s, lambda h, s=s: hop(h, s))

        when_head(t - half, lambda h: (hop(h, half), finish(h)))
        when_head(t - half + 1, attend_most)

    lax.fori_loop(0, heads + half, round_, None)

    def store(i):
        rows = pl.ds(i * 64, 64)
        return pltpu.make_async_copy(x_v.at[rows, :], out_ref.at[rows, :], wsem.at[0, i])

    for i in range(own // 64):
        x_v[i * 64 : (i + 1) * 64, :] = y_v[i * 64 : (i + 1) * 64, :].astype(bf)
        store(i).start()
    for i in range(own // 64):
        store(i).wait()

    def drain(h, _):
        for s in range(half):
            for up in (True, False):
                @pl.when(sends(s, up))
                def _():
                    send(h, s, up).wait_send()

    lax.fori_loop(0, heads, drain, None)


def solution(mesh):
    n = mesh.shape["sp"]

    def step(x, gain, wq, wk, wv, wo):
        own, d = x.shape
        heads = wk.shape[1] // HEAD
        group = wq.shape[1] // wk.shape[1]
        place = lax.axis_index("sp") * own + jnp.arange(own)
        turn = HEAD // 2
        angle = place.astype(jnp.float32)[:, None] * THETA ** (-jnp.arange(turn, dtype=jnp.float32) / turn)
        cos, sin = jnp.cos(angle), jnp.sin(angle)
        cos, sin = jnp.concatenate([cos, cos], 1), jnp.concatenate([-sin, sin], 1)
        anywhere, vmem = pl.BlockSpec(memory_space=pl.ANY), pl.BlockSpec(memory_space=pltpu.VMEM)
        bf, f32 = jnp.bfloat16, jnp.float32
        gw = group * HEAD
        return pl.pallas_call(
            functools.partial(_kernel, n, heads, group),
            out_shape=jax.ShapeDtypeStruct((own, d), bf),
            in_specs=[vmem, vmem, vmem] + [anywhere] * 5,
            out_specs=anywhere,
            scratch_shapes=[
                pltpu.VMEM((own, d), bf),
                pltpu.VMEM((own, d), bf),
                pltpu.VMEM((heads, HEAD, group * own), bf),
                pltpu.VMEM((heads, n, 2, own, HEAD), bf),
                pltpu.VMEM((own, d), f32),
                pltpu.VMEM((1, group * own), f32),
                pltpu.VMEM((HEAD + 8, group * own), f32),
                pltpu.VMEM((own, gw), bf),
                pltpu.VMEM((own, 128), f32),
                pltpu.VMEM((SLOTS, gw // WIDE * d, WIDE), bf),
                pltpu.SemaphoreType.DMA((SLOTS, d // WIDE)),
                pltpu.SemaphoreType.DMA((1,)),
                pltpu.SemaphoreType.DMA((2, heads, n // 2)),
                pltpu.SemaphoreType.DMA((2, heads, n // 2)),
            ],
            compiler_params=pltpu.CompilerParams(collective_id=0, has_side_effects=True, vmem_limit_bytes=63 * 2**20),
        )(cos, sin, gain.reshape(1, d), x, wq, wk, wv, wo)

    tokens, whole = P(("dp", "sp"), None), P(None, None)
    return jax.shard_map(
        step,
        mesh=mesh,
        in_specs=(tokens, P(None), whole, whole, whole, whole),
        out_specs=tokens,
        check_vma=False,
    )
```

```python
import functools

import jax
import jax.numpy as jnp
import numpy as np
from jax import lax
from jax.experimental import pallas as pl
from jax.experimental.pallas import tpu as pltpu
from jax.sharding import PartitionSpec as P

HEAD = 128
THETA = 10000
LOG2E = 1.4426950408889634
HIDDEN = -2e30
WIDE = 256
STRIP = 512
SLOTS = 4
AHEAD = 3


def _dot(a, b):
    return lax.dot_general(a, b, (((1,), (0,)), ((), ())), preferred_element_type=jnp.float32)


def _kernel(n, heads, group, turn_hbm, gain_hbm, x_hbm, wq, wk, wv, wo, out_ref,
            turn_v, cos_ref, sin_ref, gain_ref, x_v, a_v, q_v, kv, y_v, top_s, mix_s, o_v, part_s, wbuf, wsem, xsem, osem, ssem, rsem):
    me = lax.axis_index("sp")
    right, left = lax.rem(me + 1, n), lax.rem(me + n - 1, n)
    own, d = x_v.shape
    half = n // 2
    pairs = heads // 2
    gw = group * HEAD
    cols = group * own
    bf = jnp.bfloat16

    def pieces(kind, i, slot):
        if kind == "kv":
            at = pl.ds(i * WIDE, WIDE)
            return [pltpu.make_async_copy(w.at[:, at], wbuf.at[slot, pl.ds(j * d, d), :], wsem.at[slot, j]) for j, w in enumerate((wk, wv))]
        if kind == "q":
            return [pltpu.make_async_copy(wq.at[:, pl.ds(pl.multiple_of(i * gw + j * WIDE, WIDE), WIDE)], wbuf.at[slot, pl.ds(j * d, d), :],
                                          wsem.at[slot, j]) for j in range(gw // WIDE)]
        return [pltpu.make_async_copy(wo.at[pl.ds(pl.multiple_of(i * gw, gw), gw), pl.ds(j * WIDE, WIDE)],
                                      wbuf.at[slot, pl.ds(j * gw, gw), :], wsem.at[slot, j]) for j in range(d // WIDE)]

    def start(kind, i, slot):
        for c in pieces(kind, i, slot):
            c.start()

    def wait(kind, i, slot):
        for c in pieces(kind, i, slot):
            c.wait()

    xin = [pltpu.make_async_copy(a, b, xsem.at[i]) for i, (a, b) in enumerate((
        (x_hbm, x_v), (gain_hbm, gain_ref), (turn_hbm.at[pl.ds(pl.multiple_of(me * own, own), own), :], turn_v)))]
    for c in xin:
        c.start()
    start("kv", 0, 0)
    start("kv", 1, 1)

    barrier = pltpu.get_barrier_semaphore()
    for who in (left, right):
        pl.semaphore_signal(barrier, inc=1, device_id={"sp": who}, device_id_type=pl.DeviceIdType.MESH)

    for c in xin:
        c.wait()

    def squares(i, _):
        rows = pl.ds(pl.multiple_of(i * 16, 16), 16)
        total = jnp.zeros((16, 128), jnp.float32)
        for c in range(0, d, 128):
            w = x_v[rows, c : c + 128].astype(jnp.float32)
            total += w * w
        part_s[rows, :] = total

    lax.fori_loop(0, own // 16, squares, None)
    part_s[...] = jnp.broadcast_to(lax.rsqrt(jnp.sum(part_s[...], -1, keepdims=True) * (1 / d) + 1e-6), part_s.shape)

    def scaled(i, _):
        rows = pl.ds(pl.multiple_of(i * 16, 16), 16)
        s = part_s[rows, :]
        for c in range(0, d, 128):
            a_v[rows, c : c + 128] = (x_v[rows, c : c + 128].astype(jnp.float32) * s * gain_ref[c : c + 128].reshape(1, 128).astype(jnp.float32)).astype(bf)

    lax.fori_loop(0, own // 16, scaled, None)
    for p in range(2, pairs):
        start("kv", p, p)
    for g in range(SLOTS - pairs):
        start("q", g, pairs + g)

    turn, other = turn_v[...], pltpu.roll(turn_v[...], HEAD // 2, 1)
    low = lax.broadcasted_iota(jnp.int32, turn.shape, 1) < HEAD // 2
    cos_ref[...] = jnp.where(low, turn, other)
    sin_ref[...] = jnp.where(low, -other, turn)

    def turned(t):
        t = t.astype(bf).astype(jnp.float32)
        return (t * cos_ref[...] + pltpu.roll(t, HEAD // 2, 1) * sin_ref[...]).astype(bf)

    def project(p):
        wait("kv", p, p)
        k = _dot(a_v[...], wbuf[p, :d, :])
        v = _dot(a_v[...], wbuf[p, d : 2 * d, :])
        for j in range(2):
            at = slice(j * HEAD, (j + 1) * HEAD)
            kv[2 * p + j, me, 0] = turned(k[:, at])
            low = v[:, at].astype(bf)
            for r in range(0, own, HEAD):
                kv[2 * p + j, me, 1, r : r + HEAD, :] = low[r : r + HEAD].T
        g = SLOTS - pairs + p
        start("q", g, p)

    def send(h, s, up):
        block = lax.rem(me - s + n, n) if up else lax.rem(me + s, n)
        ref = kv.at[h, block]
        if s == half - 1:
            ref = ref.at[0 if up else 1]
        return pltpu.make_async_remote_copy(src_ref=ref, dst_ref=ref, send_sem=ssem.at[int(up), h, s], recv_sem=rsem.at[int(up), h, s],
                                            device_id={"sp": right if up else left}, device_id_type=pl.DeviceIdType.MESH)

    def arrival(h, s, up):
        block = lax.rem(me - 1 - s + n, n) if up else lax.rem(me + 1 + s, n)
        ref = kv.at[h, block]
        if s == half - 1:
            ref = ref.at[0 if up else 1]
        return pltpu.make_async_remote_copy(src_ref=ref, dst_ref=ref, send_sem=ssem.at[int(up), h, s], recv_sem=rsem.at[int(up), h, s],
                                            device_id={"sp": left if up else right}, device_id_type=pl.DeviceIdType.MESH)

    def sends(s, up):
        return (me >= s) & (me < n - 1) if up else lax.rem(me + s, n) < half

    def receives(s, up):
        return me >= s + 1 if up else lax.rem(me + 1 + s, n) < half

    def hop(h, s):
        if s == 0:
            @pl.when(h + AHEAD < heads)
            def _():
                own_hop(h + AHEAD)
            return
        for up in (True, False):
            @pl.when(receives(s - 1, up))
            def _():
                arrival(h, s - 1, up).wait_recv()
            if s < half:
                @pl.when(sends(s, up))
                def _():
                    send(h, s, up).start()

    def own_hop(h):
        for up in (True, False):
            @pl.when(sends(0, up))
            def _():
                send(h, 0, up).start()

    project(0)
    pl.semaphore_wait(barrier, 2)
    own_hop(0)
    own_hop(1)
    project(1)
    for h in range(2, AHEAD):
        own_hop(h)
    for p in range(2, pairs):
        project(p)

    def residual(i, _):
        rows = pl.ds(pl.multiple_of(i * 16, 16), 16)
        y_v[rows, :] = x_v[rows, :].astype(jnp.float32)

    lax.fori_loop(0, own // 16, residual, None)

    def queries(g):
        slot = lax.rem(pairs + g, SLOTS)
        wait("q", g, slot)
        for c in range(gw // WIDE):
            q = _dot(a_v[...], wbuf[slot, c * d : (c + 1) * d, :])
            for j in range(WIDE // HEAD):
                at = c * (WIDE // HEAD) + j
                q_v[g, :, at * own : (at + 1) * own] = turned(q[:, j * HEAD : (j + 1) * HEAD]).T
        nxt = g + SLOTS

        @pl.when(nxt < heads)
        def _():
            start("q", nxt, slot)

        @pl.when(nxt >= heads)
        def _():
            start("o", nxt - heads, slot)

    e = HEAD**-0.5 * LOG2E

    def attend(hs, blocks, first):
        pieces = [(i, at) for i in range(len(hs)) for at in range(0, cols, STRIP)]
        slots = [lax.rem(h, half + 2) for h in hs]
        scores = [[_dot(kv[hs[i], b, 0], q_v[hs[i], :, at : at + STRIP]) for b in blocks] for i, at in pieces]
        weights, keeps = [], []
        for (i, at), parts in zip(pieces, scores):
            if first:
                query = lax.rem(lax.broadcasted_iota(jnp.int32, parts[0].shape, 1), own)
                parts = [jnp.where(query >= lax.broadcasted_iota(jnp.int32, s.shape, 0), s, HIDDEN) for s in parts]
            top = functools.reduce(jnp.maximum, [s.max(axis=0, keepdims=True) for s in parts])
            if not first:
                old = top_s[slots[i], :, at : at + STRIP]
                top = jnp.maximum(old, top)
                keeps.append(jnp.exp2((old - top) * e))
            top_s[slots[i], :, at : at + STRIP] = top
            weights.append(jnp.concatenate([jnp.exp2((s - top) * e).astype(bf) for s in parts], axis=0))
        ones = jnp.ones((8, own * len(blocks)), bf)
        for j, (i, at) in enumerate(pieces):
            values = jnp.concatenate([kv[hs[i], b, 1, r : r + HEAD, :] for b in blocks for r in range(0, own, HEAD)], axis=1)
            new = _dot(jnp.concatenate([values, ones], axis=0), weights[j])
            mix_s[slots[i], :, at : at + STRIP] = new if first else mix_s[slots[i], :, at : at + STRIP] * keeps[j] + new

    def attend_arrived(r, s):
        hs = (2 * r, 2 * r + 1)

        @pl.when(me >= n - s)
        def _():
            attend(hs, (me - s, me - (n - s)), False)

        @pl.when((me >= s) & (me < n - s))
        def _():
            attend(hs, (me - s,), False)

    def result(i):
        at = pl.ds(i * 2 * WIDE, 2 * WIDE)
        return pltpu.make_async_copy(x_v.at[:, at], out_ref.at[:, at], osem.at[i])

    def finish(h):
        hop(h, half)

        @pl.when(me >= half)
        def _():
            attend((h,), (me - half,), False)

        at_h = lax.rem(h, half + 2)
        for j in range(group):
            at = slice(j * own, (j + 1) * own)
            o = mix_s[at_h, :HEAD, at] * (1 / mix_s[at_h, HEAD : HEAD + 1, at])
            o_v[:, j * HEAD : (j + 1) * HEAD] = o.astype(bf).T
        slot = lax.rem(pairs + heads + h, SLOTS)
        wait("o", h, slot)

        def out(last):
            for i in range(d // WIDE // 2):
                w = jnp.concatenate([wbuf[slot, (2 * i + j) * gw : (2 * i + j + 1) * gw, :] for j in range(2)], axis=1)
                at = slice(i * 2 * WIDE, (i + 1) * 2 * WIDE)
                y = y_v[:, at] + _dot(o_v[...], w)
                if last:
                    x_v[:, at] = y.astype(bf)
                    result(i).start()
                else:
                    y_v[:, at] = y

        @pl.when(h < heads - 1)
        def _():
            out(False)

        @pl.when(h == heads - 1)
        def _():
            out(True)

        @pl.when(h + SLOTS < heads)
        def _():
            start("o", h + SLOTS, slot)

    def when_head(h, do):
        @pl.when((h >= 0) & (h < heads))
        def _():
            do(h)

    per = 2

    def round_(t, _):
        when_head(t, lambda h: hop(h, 0))
        for i in range(per):
            when_head(t * per + i, queries)
            if i + 1 < half:
                when_head(t - i - 1, lambda h, i=i: hop(h, i + 1))

        def part(i, _):
            @pl.when(i == half // 2 - 1)
            def _():
                for s in range(per + 1, half):
                    when_head(t - s, lambda h, s=s: hop(h, s))

            s = 2 * i + 1 - lax.rem(t, 2)
            r = lax.div(t - 1 - s, 2)
            there = (t - 1 - s >= 0) & (r < pairs)

            @pl.when(there & (s == 0))
            def _():
                attend((2 * r, 2 * r + 1), (me,), True)

            @pl.when(there & (s > 0))
            def _():
                attend_arrived(r, s)

        lax.fori_loop(0, half // 2, part, None)
        when_head(t - half, finish)

    lax.fori_loop(0, heads + half, round_, None)

    for i in range(d // WIDE // 2):
        result(i).wait()

    def drain(h, _):
        for s in range(half):
            for up in (True, False):
                @pl.when(sends(s, up))
                def _():
                    send(h, s, up).wait_send()

    lax.fori_loop(0, heads, drain, None)


def solution(mesh):
    n = mesh.shape["sp"]

    def step(x, gain, wq, wk, wv, wo):
        own, d = x.shape
        heads = wk.shape[1] // HEAD
        group = wq.shape[1] // wk.shape[1]
        angle = np.arange(n * own)[:, None] * float(THETA) ** (-np.arange(HEAD // 2) / (HEAD // 2))
        turn = jnp.asarray(np.concatenate([np.cos(angle), np.sin(angle)], 1), jnp.float32)
        anywhere = pl.BlockSpec(memory_space=pl.ANY)
        bf, f32 = jnp.bfloat16, jnp.float32
        gw = group * HEAD
        return pl.pallas_call(
            functools.partial(_kernel, n, heads, group),
            out_shape=jax.ShapeDtypeStruct((own, d), bf),
            in_specs=[anywhere] * 7,
            out_specs=anywhere,
            scratch_shapes=[
                pltpu.VMEM((own, HEAD), f32),
                pltpu.VMEM((own, HEAD), f32),
                pltpu.VMEM((own, HEAD), f32),
                pltpu.VMEM((d,), bf),
                pltpu.VMEM((own, d), bf),
                pltpu.VMEM((own, d), bf),
                pltpu.VMEM((heads, HEAD, group * own), bf),
                pltpu.VMEM((heads, n, 2, own, HEAD), bf),
                pltpu.VMEM((own, d), f32),
                pltpu.VMEM((n // 2 + 2, 1, group * own), f32),
                pltpu.VMEM((n // 2 + 2, HEAD + 8, group * own), f32),
                pltpu.VMEM((own, gw), bf),
                pltpu.VMEM((own, 128), f32),
                pltpu.VMEM((SLOTS, gw // WIDE * d, WIDE), bf),
                pltpu.SemaphoreType.DMA((SLOTS, d // WIDE)),
                pltpu.SemaphoreType.DMA((3,)),
                pltpu.SemaphoreType.DMA((d // WIDE // 2,)),
                pltpu.SemaphoreType.DMA((2, heads, n // 2)),
                pltpu.SemaphoreType.DMA((2, heads, n // 2)),
            ],
            compiler_params=pltpu.CompilerParams(collective_id=0, has_side_effects=True, vmem_limit_bytes=63 * 2**20),
        )(turn, gain, x, wq, wk, wv, wo)

    tokens, whole = P(("dp", "sp"), None), P(None, None)
    return jax.shard_map(
        step,
        mesh=mesh,
        in_specs=(tokens, P(None), whole, whole, whole, whole),
        out_specs=tokens,
        check_vma=False,
    )
```

```python
import functools
import math

import jax
import jax.numpy as jnp
from jax import lax
from jax.experimental import pallas as pl
from jax.experimental.pallas import tpu as pltpu
from jax.sharding import PartitionSpec as P

HEAD = 128
THETA = 10000
LOG2E = 1.4426950408889634
HIDDEN = -2e30
WIDE = 256
STRIP = 512
SLOTS = 3
GRANT = 50 * 2**20
PARTS = 4
AHEAD = 3


def _dot(a, b):
    return lax.dot_general(a, b, (((1,), (0,)), ((), ())), preferred_element_type=jnp.float32)


def _kernel(n, heads, group, gain_hbm, x_hbm, wq, wk, wv, wo, out_ref,
            cos_ref, sin_ref, gain_ref, x_v, a_v, q_v, kv, y_v, top_s, mix_s, o_v, part_s, wbuf, wsem, xsem, ssem, rsem):
    me = lax.axis_index("sp")
    right, left = lax.rem(me + 1, n), lax.rem(me + n - 1, n)
    own, d = x_v.shape
    half = n // 2
    pairs = heads // 2
    gw = group * HEAD
    cols = group * own
    bf = jnp.bfloat16

    def pieces(kind, i, slot):
        if kind == "kv":
            at = pl.ds(i * WIDE, WIDE)
            return [pltpu.make_async_copy(w.at[:, at], wbuf.at[slot, pl.ds(j * d, d), :], wsem.at[slot, j]) for j, w in enumerate((wk, wv))]
        if kind == "q":
            return [pltpu.make_async_copy(wq.at[:, pl.ds(pl.multiple_of(i * gw + j * WIDE, WIDE), WIDE)], wbuf.at[slot, pl.ds(j * d, d), :],
                                          wsem.at[slot, j]) for j in range(gw // WIDE)]
        return [pltpu.make_async_copy(wo.at[pl.ds(pl.multiple_of(i * gw, gw), gw), pl.ds(j * WIDE, WIDE)],
                                      wbuf.at[slot, pl.ds(j * gw, gw), :], wsem.at[slot, j]) for j in range(d // WIDE)]

    def start(kind, i, slot):
        for c in pieces(kind, i, slot):
            c.start()

    def wait(kind, i, slot):
        for c in pieces(kind, i, slot):
            c.wait()

    gains = pltpu.make_async_copy(gain_hbm, gain_ref, xsem.at[PARTS])
    part = own // PARTS
    tokens = [pltpu.make_async_copy(x_hbm.at[pl.ds(i * part, part), :], x_v.at[pl.ds(i * part, part), :], xsem.at[i]) for i in range(PARTS)]
    for c in tokens + [gains]:
        c.start()
    start("kv", 0, 0)
    start("kv", 1, 1)

    barrier = pltpu.get_barrier_semaphore()
    for who in (left, right):
        pl.semaphore_signal(barrier, inc=1, device_id={"sp": who}, device_id_type=pl.DeviceIdType.MESH)

    turn = HEAD // 2

    def angles(i, _):
        rows = pl.ds(pl.multiple_of(i * 64, 64), 64)
        lane = lax.broadcasted_iota(jnp.int32, (64, HEAD), 1)
        place = me * own + i * 64 + lax.broadcasted_iota(jnp.int32, (64, HEAD), 0)
        angle = place.astype(jnp.float32) * jnp.exp(lax.rem(lane, turn).astype(jnp.float32) * (-math.log(THETA) / turn))
        sin = jnp.sin(angle)
        cos_ref[rows, :] = jnp.cos(angle)
        sin_ref[rows, :] = jnp.where(lane < turn, -sin, sin)

    lax.fori_loop(0, own // 64, angles, None)


    def squares(i, _):
        rows = pl.ds(pl.multiple_of(i * 16, 16), 16)
        total = jnp.zeros((16, 128), jnp.float32)
        for c in range(0, d, 128):
            w = x_v[rows, c : c + 128].astype(jnp.float32)
            total += w * w
        part_s[rows, :] = total

    for i, c in enumerate(tokens):
        c.wait()
        lax.fori_loop(i * part // 16, (i + 1) * part // 16, squares, None)
    gains.wait()
    part_s[...] = jnp.broadcast_to(lax.rsqrt(jnp.sum(part_s[...], -1, keepdims=True) * (1 / d) + 1e-6), part_s.shape)

    def scaled(i, _):
        rows = pl.ds(pl.multiple_of(i * 16, 16), 16)
        s = part_s[rows, :]
        for c in range(0, d, 128):
            a_v[rows, c : c + 128] = (x_v[rows, c : c + 128].astype(jnp.float32) * s * gain_ref[c : c + 128].reshape(1, 128).astype(jnp.float32)).astype(bf)

    lax.fori_loop(0, own // 16, scaled, None)
    for p in range(2, SLOTS):
        start("kv", p, p)

    def turned(t):
        t = t.astype(bf).astype(jnp.float32)
        return (t * cos_ref[...] + pltpu.roll(t, turn, 1) * sin_ref[...]).astype(bf)

    def project(p):
        slot = p % SLOTS
        wait("kv", p, slot)
        k = _dot(a_v[...], wbuf[slot, :d, :])
        v = _dot(a_v[...], wbuf[slot, d : 2 * d, :])
        for j in range(2):
            at = slice(j * HEAD, (j + 1) * HEAD)
            kv[2 * p + j, me, 0] = turned(k[:, at])
            low = v[:, at].astype(bf)
            for r in range(0, own, HEAD):
                kv[2 * p + j, me, 1, r : r + HEAD, :] = low[r : r + HEAD].T
        start(*(("kv", p + SLOTS) if p + SLOTS < pairs else ("q", p + SLOTS - pairs)), slot)

    def send(h, s, up):
        block = lax.rem(me - s + n, n) if up else lax.rem(me + s, n)
        ref = kv.at[h, block]
        if s == half - 1:
            ref = ref.at[0 if up else 1]
        return pltpu.make_async_remote_copy(src_ref=ref, dst_ref=ref, send_sem=ssem.at[int(up), h, s], recv_sem=rsem.at[int(up), h, s],
                                            device_id={"sp": right if up else left}, device_id_type=pl.DeviceIdType.MESH)

    def arrival(h, s, up):
        block = lax.rem(me - 1 - s + n, n) if up else lax.rem(me + 1 + s, n)
        ref = kv.at[h, block]
        if s == half - 1:
            ref = ref.at[0 if up else 1]
        return pltpu.make_async_remote_copy(src_ref=ref, dst_ref=ref, send_sem=ssem.at[int(up), h, s], recv_sem=rsem.at[int(up), h, s],
                                            device_id={"sp": left if up else right}, device_id_type=pl.DeviceIdType.MESH)

    def sends(s, up):
        return (me >= s) & (me < n - 1) if up else lax.rem(me + s, n) < half

    def receives(s, up):
        return me >= s + 1 if up else lax.rem(me + 1 + s, n) < half

    def hop(h, s):
        if s == 0:
            @pl.when(h + AHEAD < heads)
            def _():
                own_hop(h + AHEAD)
            return
        for up in (True, False):
            @pl.when(receives(s - 1, up))
            def _():
                arrival(h, s - 1, up).wait_recv()
            if s < half:
                @pl.when(sends(s, up))
                def _():
                    send(h, s, up).start()

    def own_hop(h):
        for up in (True, False):
            @pl.when(sends(0, up))
            def _():
                send(h, 0, up).start()

    project(0)
    pl.semaphore_wait(barrier, 2)
    own_hop(0)
    own_hop(1)
    project(1)
    for h in range(2, AHEAD):
        own_hop(h)
    for p in range(2, pairs):
        project(p)

    def residual(i, _):
        rows = pl.ds(pl.multiple_of(i * 16, 16), 16)
        y_v[rows, :] = x_v[rows, :].astype(jnp.float32)

    lax.fori_loop(0, own // 16, residual, None)

    def queries(g):
        slot = lax.rem(pairs + g, SLOTS)
        wait("q", g, slot)
        for c in range(gw // WIDE):
            q = _dot(a_v[...], wbuf[slot, c * d : (c + 1) * d, :])
            for j in range(WIDE // HEAD):
                at = c * (WIDE // HEAD) + j
                q_v[g, :, at * own : (at + 1) * own] = turned(q[:, j * HEAD : (j + 1) * HEAD]).T
        nxt = g + SLOTS

        @pl.when(nxt < heads)
        def _():
            start("q", nxt, slot)

        @pl.when(nxt >= heads)
        def _():
            start("o", nxt - heads, slot)

    e = HEAD**-0.5 * LOG2E

    def attend(hs, blocks, first):
        pieces = [(i, at) for i in range(len(hs)) for at in range(0, cols, STRIP)]
        slots = [lax.rem(h, half + 2) for h in hs]
        scores = [[_dot(kv[hs[i], b, 0], q_v[hs[i], :, at : at + STRIP]) for b in blocks] for i, at in pieces]
        weights, keeps = [], []
        for (i, at), parts in zip(pieces, scores):
            if first:
                query = lax.rem(lax.broadcasted_iota(jnp.int32, parts[0].shape, 1), own)
                parts = [jnp.where(query >= lax.broadcasted_iota(jnp.int32, s.shape, 0), s, HIDDEN) for s in parts]
            top = functools.reduce(jnp.maximum, [s.max(axis=0, keepdims=True) for s in parts])
            if not first:
                old = top_s[slots[i], :, at : at + STRIP]
                top = jnp.maximum(old, top)
                keeps.append(jnp.exp2((old - top) * e))
            top_s[slots[i], :, at : at + STRIP] = top
            weights.append(jnp.concatenate([jnp.exp2((s - top) * e).astype(bf) for s in parts], axis=0))
        ones = jnp.ones((8, own * len(blocks)), bf)
        for j, (i, at) in enumerate(pieces):
            values = jnp.concatenate([kv[hs[i], b, 1, r : r + HEAD, :] for b in blocks for r in range(0, own, HEAD)], axis=1)
            new = _dot(jnp.concatenate([values, ones], axis=0), weights[j])
            mix_s[slots[i], :, at : at + STRIP] = new if first else mix_s[slots[i], :, at : at + STRIP] * keeps[j] + new

    def attend_arrived(r, s):
        hs = (2 * r, 2 * r + 1)

        @pl.when(me >= n - s)
        def _():
            attend(hs, (me - s, me - (n - s)), False)

        @pl.when((me >= s) & (me < n - s))
        def _():
            attend(hs, (me - s,), False)

    def finish(h):
        hop(h, half)

        @pl.when(me >= half)
        def _():
            attend((h,), (me - half,), False)

        at_h = lax.rem(h, half + 2)
        for j in range(group):
            at = slice(j * own, (j + 1) * own)
            o = mix_s[at_h, :HEAD, at] * (1 / mix_s[at_h, HEAD : HEAD + 1, at])
            o_v[:, j * HEAD : (j + 1) * HEAD] = o.astype(bf).T
        slot = lax.rem(pairs + heads + h, SLOTS)
        wait("o", h, slot)

        def out(last):
            for i in range(d // WIDE // 2):
                w = jnp.concatenate([wbuf[slot, (2 * i + j) * gw : (2 * i + j + 1) * gw, :] for j in range(2)], axis=1)
                at = slice(i * 2 * WIDE, (i + 1) * 2 * WIDE)
                y = y_v[:, at] + _dot(o_v[...], w)
                if last:
                    out_ref[:, at] = y.astype(bf)
                else:
                    y_v[:, at] = y

        @pl.when(h < heads - 1)
        def _():
            out(False)

        @pl.when(h == heads - 1)
        def _():
            out(True)

        @pl.when(h + SLOTS < heads)
        def _():
            start("o", h + SLOTS, slot)

    def when_head(h, do):
        @pl.when((h >= 0) & (h < heads))
        def _():
            do(h)

    per = 2

    def round_(t, _):
        when_head(t, lambda h: hop(h, 0))
        for i in range(per):
            when_head(t * per + i, queries)
            if i + 1 < half:
                when_head(t - i - 1, lambda h, i=i: hop(h, i + 1))

        def part(i, _):
            @pl.when(i == half // 2 - 1)
            def _():
                for s in range(per + 1, half):
                    when_head(t - s, lambda h, s=s: hop(h, s))

            s = 2 * i + 1 - lax.rem(t, 2)
            r = lax.div(t - 1 - s, 2)
            there = (t - 1 - s >= 0) & (r < pairs)

            @pl.when(there & (s == 0))
            def _():
                attend((2 * r, 2 * r + 1), (me,), True)

            @pl.when(there & (s > 0))
            def _():
                attend_arrived(r, s)

        lax.fori_loop(0, half // 2, part, None)
        when_head(t - half, finish)

    lax.fori_loop(0, heads + half, round_, None)

    def drain(h, _):
        for s in range(half):
            for up in (True, False):
                @pl.when(sends(s, up))
                def _():
                    send(h, s, up).wait_send()

    lax.fori_loop(0, heads, drain, None)


def solution(mesh):
    n = mesh.shape["sp"]

    def step(x, gain, wq, wk, wv, wo):
        own, d = x.shape
        heads = wk.shape[1] // HEAD
        group = wq.shape[1] // wk.shape[1]
        anywhere = pl.BlockSpec(memory_space=pl.ANY)
        bf, f32 = jnp.bfloat16, jnp.float32
        gw = group * HEAD
        return pl.pallas_call(
            functools.partial(_kernel, n, heads, group),
            out_shape=jax.ShapeDtypeStruct((own, d), bf),
            in_specs=[anywhere] * 6,
            out_specs=pl.BlockSpec(memory_space=pltpu.VMEM),
            scratch_shapes=[
                pltpu.VMEM((own, HEAD), f32),
                pltpu.VMEM((own, HEAD), f32),
                pltpu.VMEM((d,), bf),
                pltpu.VMEM((own, d), bf),
                pltpu.VMEM((own, d), bf),
                pltpu.VMEM((heads, HEAD, group * own), bf),
                pltpu.VMEM((heads, n, 2, own, HEAD), bf),
                pltpu.VMEM((own, d), f32),
                pltpu.VMEM((n // 2 + 2, 1, group * own), f32),
                pltpu.VMEM((n // 2 + 2, HEAD + 8, group * own), f32),
                pltpu.VMEM((own, gw), bf),
                pltpu.VMEM((own, 128), f32),
                pltpu.VMEM((SLOTS, gw // WIDE * d, WIDE), bf),
                pltpu.SemaphoreType.DMA((SLOTS, d // WIDE)),
                pltpu.SemaphoreType.DMA((PARTS + 1,)),
                pltpu.SemaphoreType.DMA((2, heads, n // 2)),
                pltpu.SemaphoreType.DMA((2, heads, n // 2)),
            ],
            compiler_params=pltpu.CompilerParams(collective_id=0, has_side_effects=True, vmem_limit_bytes=GRANT),
        )(gain, x, wq, wk, wv, wo)

    tokens, whole = P(("dp", "sp"), None), P(None, None)
    return jax.shard_map(
        step,
        mesh=mesh,
        in_specs=(tokens, P(None), whole, whole, whole, whole),
        out_specs=tokens,
        check_vma=False,
    )
```

```python
import functools
import math

import jax
import jax.numpy as jnp
from jax import lax
from jax.experimental import pallas as pl
from jax.experimental.pallas import tpu as pltpu
from jax.sharding import PartitionSpec as P

HEAD = 128
THETA = 10000
LOG2E = 1.4426950408889634
HIDDEN = -2e30
WIDE = 256
STRIP = 512
SLOTS = 3
GRANT = 50 * 2**20
PARTS = 4
AHEAD = 3


def _dot(a, b):
    return lax.dot_general(a, b, (((1,), (0,)), ((), ())), preferred_element_type=jnp.float32)


def _kernel(n, heads, group, gain_hbm, x_hbm, wq, wk, wv, wo, out_ref,
            cos_ref, sin_ref, gain_ref, x_v, a_v, q_v, kv, y_v, top_s, mix_s, o_v, part_s, wbuf, wsem, xsem, ssem, rsem):
    me = lax.axis_index("sp")
    right, left = lax.rem(me + 1, n), lax.rem(me + n - 1, n)
    own, d = x_v.shape
    half = n // 2
    pairs = heads // 2
    gw = group * HEAD
    cols = group * own
    bf = jnp.bfloat16

    def pieces(kind, i, slot):
        if kind == "kv":
            at = pl.ds(i * WIDE, WIDE)
            return [pltpu.make_async_copy(w.at[:, at], wbuf.at[slot, pl.ds(j * d, d), :], wsem.at[slot, j]) for j, w in enumerate((wk, wv))]
        if kind == "q":
            return [pltpu.make_async_copy(wq.at[:, pl.ds(pl.multiple_of(i * gw + j * WIDE, WIDE), WIDE)], wbuf.at[slot, pl.ds(j * d, d), :],
                                          wsem.at[slot, j]) for j in range(gw // WIDE)]
        return [pltpu.make_async_copy(wo.at[pl.ds(pl.multiple_of(i * gw, gw), gw), pl.ds(j * WIDE, WIDE)],
                                      wbuf.at[slot, pl.ds(j * gw, gw), :], wsem.at[slot, j]) for j in range(d // WIDE)]

    def start(kind, i, slot):
        for c in pieces(kind, i, slot):
            c.start()

    def wait(kind, i, slot):
        for c in pieces(kind, i, slot):
            c.wait()

    gains = pltpu.make_async_copy(gain_hbm, gain_ref, xsem.at[PARTS])
    part = own // PARTS
    tokens = [pltpu.make_async_copy(x_hbm.at[pl.ds(i * part, part), :], x_v.at[pl.ds(i * part, part), :], xsem.at[i]) for i in range(PARTS)]
    for c in tokens + [gains]:
        c.start()
    start("kv", 0, 0)
    start("kv", 1, 1)

    barrier = pltpu.get_barrier_semaphore()
    for who in (left, right):
        pl.semaphore_signal(barrier, inc=1, device_id={"sp": who}, device_id_type=pl.DeviceIdType.MESH)

    turn = HEAD // 2

    def angles(i, _):
        rows = pl.ds(pl.multiple_of(i * 64, 64), 64)
        lane = lax.broadcasted_iota(jnp.int32, (64, HEAD), 1)
        place = me * own + i * 64 + lax.broadcasted_iota(jnp.int32, (64, HEAD), 0)
        angle = place.astype(jnp.float32) * jnp.exp(lax.rem(lane, turn).astype(jnp.float32) * (-math.log(THETA) / turn))
        sin = jnp.sin(angle)
        cos_ref[rows, :] = jnp.cos(angle)
        sin_ref[rows, :] = jnp.where(lane < turn, -sin, sin)

    lax.fori_loop(0, own // 64, angles, None)


    def squares(i, _):
        rows = pl.ds(pl.multiple_of(i * 16, 16), 16)
        total = jnp.zeros((16, 128), jnp.float32)
        for c in range(0, d, 128):
            w = x_v[rows, c : c + 128].astype(jnp.float32)
            total += w * w
        part_s[rows, :] = total

    for i, c in enumerate(tokens):
        c.wait()
        lax.fori_loop(i * part // 16, (i + 1) * part // 16, squares, None)
    gains.wait()
    part_s[...] = jnp.broadcast_to(lax.rsqrt(jnp.sum(part_s[...], -1, keepdims=True) * (1 / d) + 1e-6), part_s.shape)

    def scaled(i, _):
        rows = pl.ds(pl.multiple_of(i * 16, 16), 16)
        s = part_s[rows, :]
        for c in range(0, d, 128):
            a_v[rows, c : c + 128] = (x_v[rows, c : c + 128].astype(jnp.float32) * s * gain_ref[c : c + 128].reshape(1, 128).astype(jnp.float32)).astype(bf)

    lax.fori_loop(0, own // 16, scaled, None)
    for p in range(2, SLOTS):
        start("kv", p, p)

    def turned(t):
        t = t.astype(bf).astype(jnp.float32)
        return (t * cos_ref[...] + pltpu.roll(t, turn, 1) * sin_ref[...]).astype(bf)

    def project(p):
        slot = p % SLOTS
        wait("kv", p, slot)
        k = _dot(a_v[...], wbuf[slot, :d, :])
        v = _dot(a_v[...], wbuf[slot, d : 2 * d, :])
        for j in range(2):
            at = slice(j * HEAD, (j + 1) * HEAD)
            kv[2 * p + j, me, 0] = turned(k[:, at])
            low = v[:, at].astype(bf)
            for r in range(0, own, HEAD):
                kv[2 * p + j, me, 1, r : r + HEAD, :] = low[r : r + HEAD].T
        start(*(("kv", p + SLOTS) if p + SLOTS < pairs else ("q", p + SLOTS - pairs)), slot)

    def send(h, s, up):
        block = lax.rem(me - s + n, n) if up else lax.rem(me + s, n)
        ref = kv.at[h, block]
        if s == half - 1:
            ref = ref.at[0 if up else 1]
        return pltpu.make_async_remote_copy(src_ref=ref, dst_ref=ref, send_sem=ssem.at[int(up), h, s], recv_sem=rsem.at[int(up), h, s],
                                            device_id={"sp": right if up else left}, device_id_type=pl.DeviceIdType.MESH)

    def arrival(h, s, up):
        block = lax.rem(me - 1 - s + n, n) if up else lax.rem(me + 1 + s, n)
        ref = kv.at[h, block]
        if s == half - 1:
            ref = ref.at[0 if up else 1]
        return pltpu.make_async_remote_copy(src_ref=ref, dst_ref=ref, send_sem=ssem.at[int(up), h, s], recv_sem=rsem.at[int(up), h, s],
                                            device_id={"sp": left if up else right}, device_id_type=pl.DeviceIdType.MESH)

    def sends(s, up):
        return (me >= s) & (me < n - 1) if up else lax.rem(me + s, n) < half

    def receives(s, up):
        return me >= s + 1 if up else lax.rem(me + 1 + s, n) < half

    def hop(h, s):
        if s == 0:
            @pl.when(h + AHEAD < heads)
            def _():
                own_hop(h + AHEAD)
            return
        for up in (True, False):
            @pl.when(receives(s - 1, up))
            def _():
                arrival(h, s - 1, up).wait_recv()
            if s < half:
                @pl.when(sends(s, up))
                def _():
                    send(h, s, up).start()

    def own_hop(h):
        for up in (True, False):
            @pl.when(sends(0, up))
            def _():
                send(h, 0, up).start()

    project(0)
    pl.semaphore_wait(barrier, 2)
    own_hop(0)
    own_hop(1)
    project(1)
    for h in range(2, AHEAD):
        own_hop(h)
    for p in range(2, pairs):
        project(p)

    def residual(i, _):
        rows = pl.ds(pl.multiple_of(i * 16, 16), 16)
        y_v[rows, :] = x_v[rows, :].astype(jnp.float32)

    lax.fori_loop(0, own // 16, residual, None)

    def queries(g):
        slot = lax.rem(pairs + g, SLOTS)
        wait("q", g, slot)
        for c in range(gw // WIDE):
            q = _dot(a_v[...], wbuf[slot, c * d : (c + 1) * d, :])
            for j in range(WIDE // HEAD):
                at = c * (WIDE // HEAD) + j
                q_v[g, :, at * own : (at + 1) * own] = turned(q[:, j * HEAD : (j + 1) * HEAD]).T
        nxt = g + SLOTS

        @pl.when(nxt < heads)
        def _():
            start("q", nxt, slot)

        @pl.when(nxt >= heads)
        def _():
            start("o", nxt - heads, slot)

    e = HEAD**-0.5 * LOG2E

    def attend(hs, blocks, first):
        pieces = [(i, at) for i in range(len(hs)) for at in range(0, cols, STRIP)]
        slots = [lax.rem(h, half + 2) for h in hs]
        scores = [[_dot(kv[hs[i], b, 0], q_v[hs[i], :, at : at + STRIP]) for b in blocks] for i, at in pieces]
        weights, keeps = [], []
        for (i, at), parts in zip(pieces, scores):
            if first:
                query = lax.rem(lax.broadcasted_iota(jnp.int32, parts[0].shape, 1), own)
                parts = [jnp.where(query >= lax.broadcasted_iota(jnp.int32, s.shape, 0), s, HIDDEN) for s in parts]
            top = functools.reduce(jnp.maximum, [s.max(axis=0, keepdims=True) for s in parts])
            if not first:
                old = top_s[slots[i], :, at : at + STRIP]
                top = jnp.maximum(old, top)
                keeps.append(jnp.exp2((old - top) * e))
            top_s[slots[i], :, at : at + STRIP] = top
            weights.append(jnp.concatenate([jnp.exp2((s - top) * e).astype(bf) for s in parts], axis=0))
        ones = jnp.ones((8, own * len(blocks)), bf)
        for j, (i, at) in enumerate(pieces):
            values = jnp.concatenate([kv[hs[i], b, 1, r : r + HEAD, :] for b in blocks for r in range(0, own, HEAD)], axis=1)
            new = _dot(jnp.concatenate([values, ones], axis=0), weights[j])
            mix_s[slots[i], :, at : at + STRIP] = new if first else mix_s[slots[i], :, at : at + STRIP] * keeps[j] + new

    def attend_arrived(r, s):
        hs = (2 * r, 2 * r + 1)

        @pl.when(me >= n - s)
        def _():
            attend(hs, (me - s, me - (n - s)), False)

        @pl.when((me >= s) & (me < n - s))
        def _():
            attend(hs, (me - s,), False)

    def finish(h):
        hop(h, half)

        @pl.when(me >= half)
        def _():
            attend((h,), (me - half,), False)

        at_h = lax.rem(h, half + 2)
        for j in range(group):
            at = slice(j * own, (j + 1) * own)
            o = mix_s[at_h, :HEAD, at] * (1 / mix_s[at_h, HEAD : HEAD + 1, at])
            o_v[:, j * HEAD : (j + 1) * HEAD] = o.astype(bf).T
        slot = lax.rem(pairs + heads + h, SLOTS)
        wait("o", h, slot)

        def out(last):
            for i in range(d // WIDE // 2):
                w = jnp.concatenate([wbuf[slot, (2 * i + j) * gw : (2 * i + j + 1) * gw, :] for j in range(2)], axis=1)
                at = slice(i * 2 * WIDE, (i + 1) * 2 * WIDE)
                y = y_v[:, at] + _dot(o_v[...], w)
                if last:
                    out_ref[:, at] = y.astype(bf)
                else:
                    y_v[:, at] = y

        @pl.when(h < heads - 1)
        def _():
            out(False)

        @pl.when(h == heads - 1)
        def _():
            out(True)

        @pl.when(h + SLOTS < heads)
        def _():
            start("o", h + SLOTS, slot)

    def when_head(h, do):
        @pl.when((h >= 0) & (h < heads))
        def _():
            do(h)

    per = 2

    def round_(t, _):
        when_head(t, lambda h: hop(h, 0))
        for i in range(per):
            when_head(t * per + i, queries)
            if i + 1 < half:
                when_head(t - i - 1, lambda h, i=i: hop(h, i + 1))

        odd = lax.rem(t, 2)

        def last_hops():
            for s in range(per + 1, half):
                when_head(t - s, lambda h, s=s: hop(h, s))

        def part(i, _):
            s = 2 * i + 1 - odd
            r = lax.div(t - 1 - s, 2)
            there = (t - 1 - s >= 0) & (r < pairs)

            @pl.when((i == half // 2 - 1) & (odd == 0))
            def _():
                last_hops()

            @pl.when(there & (s == 0))
            def _():
                attend((2 * r, 2 * r + 1), (me,), True)

            @pl.when(there & (s > 0))
            def _():
                attend_arrived(r, s)

            @pl.when((i == half // 2 - 1) & (odd == 1))
            def _():
                last_hops()

        lax.fori_loop(0, half // 2, part, None)
        when_head(t - half, finish)

    lax.fori_loop(0, heads + half, round_, None)

    def drain(h, _):
        for s in range(half):
            for up in (True, False):
                @pl.when(sends(s, up))
                def _():
                    send(h, s, up).wait_send()

    lax.fori_loop(0, heads, drain, None)


def solution(mesh):
    n = mesh.shape["sp"]

    def step(x, gain, wq, wk, wv, wo):
        own, d = x.shape
        heads = wk.shape[1] // HEAD
        group = wq.shape[1] // wk.shape[1]
        anywhere = pl.BlockSpec(memory_space=pl.ANY)
        bf, f32 = jnp.bfloat16, jnp.float32
        gw = group * HEAD
        return pl.pallas_call(
            functools.partial(_kernel, n, heads, group),
            out_shape=jax.ShapeDtypeStruct((own, d), bf),
            in_specs=[anywhere] * 6,
            out_specs=pl.BlockSpec(memory_space=pltpu.VMEM),
            scratch_shapes=[
                pltpu.VMEM((own, HEAD), f32),
                pltpu.VMEM((own, HEAD), f32),
                pltpu.VMEM((d,), bf),
                pltpu.VMEM((own, d), bf),
                pltpu.VMEM((own, d), bf),
                pltpu.VMEM((heads, HEAD, group * own), bf),
                pltpu.VMEM((heads, n, 2, own, HEAD), bf),
                pltpu.VMEM((own, d), f32),
                pltpu.VMEM((n // 2 + 2, 1, group * own), f32),
                pltpu.VMEM((n // 2 + 2, HEAD + 8, group * own), f32),
                pltpu.VMEM((own, gw), bf),
                pltpu.VMEM((own, 128), f32),
                pltpu.VMEM((SLOTS, gw // WIDE * d, WIDE), bf),
                pltpu.SemaphoreType.DMA((SLOTS, d // WIDE)),
                pltpu.SemaphoreType.DMA((PARTS + 1,)),
                pltpu.SemaphoreType.DMA((2, heads, n // 2)),
                pltpu.SemaphoreType.DMA((2, heads, n // 2)),
            ],
            compiler_params=pltpu.CompilerParams(collective_id=0, has_side_effects=True, vmem_limit_bytes=GRANT),
        )(gain, x, wq, wk, wv, wo)

    tokens, whole = P(("dp", "sp"), None), P(None, None)
    return jax.shard_map(
        step,
        mesh=mesh,
        in_specs=(tokens, P(None), whole, whole, whole, whole),
        out_specs=tokens,
        check_vma=False,
    )
```
